16 devices in a mesh: dp: 1, tp: 16 (over x, y, z, core).
Axes of the slice: x: 2, y: 2, z: 2, core: 2. Of those that a mesh axis runs over, the one named last changes fastest.
Arguments:
- x: bfloat16 [5120, 3584], P(('dp', 'tp'))
- dy: bfloat16 [5120, 3584], P(('dp', 'tp'))
- gate: bfloat16 [5120, 14336], P('dp', 'tp')
- up: bfloat16 [5120, 14336], P('dp', 'tp')
- w_gate: bfloat16 [3584, 14336], P(None, 'tp')
- w_up: bfloat16 [3584, 14336], P(None, 'tp')
- w_down: bfloat16 [14336, 3584], P('tp')
Outputs:
- output 1: bfloat16 [5120, 3584], P(('dp', 'tp'))
- output 2: bfloat16 [3584, 14336], P('dp', 'tp')
- output 3: bfloat16 [3584, 14336], P('dp', 'tp')
- output 4: bfloat16 [14336, 3584], P(('dp', 'tp'))
All inputs are finite; a program needn't handle non-finite values.
Results may differ from the reference program's by a relative error of at most 0.012.
Values are sent between devices in bfloat16 or wider.
A program may use at most 2 GiB of HBM per device.

```python
import jax
import jax.numpy as jnp

ROWS = 5120
D = 3584
FF = 14336


def act(gate, up):
    return jax.nn.gelu(gate) * up


def setup_inputs(seed: int = 0, part: int = 0) -> dict:
    kx, ky, ka, kb, kg, ku, kd = jax.random.split(jax.random.key(seed), 7)
    kx, ky, ka, kb = (jax.random.fold_in(k, part) for k in (kx, ky, ka, kb))
    drawn = {
        "x": jax.random.normal(kx, (ROWS, D), jnp.float32),
        "dy": jax.random.normal(ky, (ROWS, D), jnp.float32),
        "gate": jax.random.normal(ka, (ROWS, FF), jnp.float32),
        "up": jax.random.normal(kb, (ROWS, FF), jnp.float32),
        "w_gate": jax.random.normal(kg, (D, FF), jnp.float32) * D**-0.5,
        "w_up": jax.random.normal(ku, (D, FF), jnp.float32) * D**-0.5,
        "w_down": jax.random.normal(kd, (FF, D), jnp.float32) * FF**-0.5,
    }
    return {k: v.astype(jnp.bfloat16) for k, v in drawn.items()}


def reference(x, dy, gate, up, w_gate, w_up, w_down):
    hidden, back = jax.vjp(act, gate.astype(jnp.float32), up.astype(jnp.float32))
    d_hidden = jnp.dot(dy, w_down.T, preferred_element_type=jnp.float32)
    d_gate, d_up = (g.astype(jnp.bfloat16) for g in back(d_hidden))
    dx = jnp.dot(d_gate, w_gate.T, preferred_element_type=jnp.float32) + jnp.dot(d_up, w_up.T, preferred_element_type=jnp.float32)
    dw_gate = jnp.dot(x.T, d_gate, preferred_element_type=jnp.float32)
    dw_up = jnp.dot(x.T, d_up, preferred_element_type=jnp.float32)
    dw_down = jnp.dot(hidden.astype(jnp.bfloat16).T, dy, preferred_element_type=jnp.float32)
    return tuple(g.astype(jnp.bfloat16) for g in (dx, dw_gate, dw_up, dw_down))
```

```python
import jax
import jax.numpy as jnp
from jax.sharding import PartitionSpec as P


def act(gate, up):
    return jax.nn.gelu(gate) * up


def solution(mesh):
    def body(x, dy, gate, up, w_gate, w_up, w_down):
        dy_all = jax.lax.all_gather(dy, "tp", axis=0, tiled=True)
        x_all = jax.lax.all_gather(x, "tp", axis=0, tiled=True)
        hidden, back = jax.vjp(act, gate.astype(jnp.float32), up.astype(jnp.float32))
        d_hidden = jax.lax.dot_general(dy_all, w_down, (((1,), (1,)), ((), ())), preferred_element_type=jnp.float32)
        d_gate, d_up = (g.astype(jnp.bfloat16) for g in back(d_hidden))
        hidden = hidden.astype(jnp.bfloat16)
        dx = jax.lax.dot_general(d_gate, w_gate, (((1,), (1,)), ((), ())), preferred_element_type=jnp.float32)
        dx = dx + jax.lax.dot_general(d_up, w_up, (((1,), (1,)), ((), ())), preferred_element_type=jnp.float32)
        dx = jax.lax.psum_scatter(dx.astype(jnp.bfloat16), "tp", scatter_dimension=0, tiled=True)

        def over_tokens(a, b):
            product = jax.lax.dot_general(a, b, (((0,), (0,)), ((), ())), preferred_element_type=jnp.float32)
            return product.astype(jnp.bfloat16)

        return dx, over_tokens(x_all, d_gate), over_tokens(x_all, d_up), over_tokens(hidden, dy_all)

    rows, cols = P(("dp", "tp"), None), P("dp", "tp")
    return jax.shard_map(
        body,
        mesh=mesh,
        in_specs=(rows, rows, cols, cols, P(None, "tp"), P(None, "tp"), P("tp", None)),
        out_specs=(rows, cols, cols, rows),
        check_vma=False,
    )
```

```python
import functools

import jax
import jax.numpy as jnp
from jax import lax
from jax.experimental import pallas as pl
from jax.experimental.pallas import tpu as pltpu
from jax.sharding import PartitionSpec as P

BF = jnp.bfloat16
F32 = jnp.float32
S = 10
R = 32
RING = 8
CHUNK = 16 * R
HALF = 8 * R
D = 3584
FL = 896
MASKS = (8, 4, 2)
BIT = (4, 2, 1)
HALVES = ((0, 1792), (1792, 1792))
THIRDS = ((0, 1152), (1152, 1280), (2432, 1152))
PAIRS = ((0, 1), (1, 2), (2, 0))
OTHERS = ((1, 2), (0, 2), (0, 1))
XYZ = 7
VMEM_LIMIT = 67_000_000


def act(gate, up):
    return jax.nn.gelu(gate) * up


def flip(me, mask):
    return me + mask * (1 - 2 * ((me // mask) % 2))


def peers_of(me):
    return [flip(me, m) for m in MASKS] + [flip(me, 1)]


def greet(peers):
    barrier = pltpu.get_barrier_semaphore()
    for peer in peers:
        pl.semaphore_signal(barrier, inc=1, device_id={"tp": peer}, device_id_type=pl.DeviceIdType.MESH)
    pl.semaphore_wait(barrier, len(peers))


def send(src, dst, send_sem, recv_sem, peer):
    return pltpu.make_async_remote_copy(
        src_ref=src, dst_ref=dst, send_sem=send_sem, recv_sem=recv_sem,
        device_id={"tp": peer}, device_id_type=pl.DeviceIdType.MESH,
    )


def gather_kernel(dy, x, gate, up, w_down, dgu, dw_gate, dw_up, dw_down, buf,
                  wd_v, acc, rows_v, gate_v, up_v, dgu_v, ht_v, stage,
                  ss, rs, load_sem, act_sem, w_sem, put_sem, out_sem):
    me = lax.axis_index("tp")
    peers = peers_of(me)
    last = 2 * S

    def place(g, v, core):
        return buf.at[g, pl.ds((core * 8 + v) * R, R)]

    def part(g, v, cols):
        return buf.at[g, pl.ds(v * R, R), pl.ds(*cols)]

    def own(g):
        return dy.at[pl.ds(g * R, R)], x.at[pl.ds((g - S) * R, R)]

    def copy(src, dst, g, k, peer):
        return send(src, dst, ss.at[g % RING, k], rs.at[g % RING, k], peer)

    def to_axis(g, d, src):
        return copy(src, place(g, BIT[d], 0), g, d, peers[d])

    def relay(g, q, h):
        a, b = PAIRS[q]
        via, src = (a, b) if h == 0 else (b, a)
        return copy(part(g, BIT[src], HALVES[h]), part(g, BIT[a] + BIT[b], HALVES[h]), g, 3 + 2 * q + h, peers[via])

    def relay_last(g, d):
        o, p = OTHERS[d]
        return copy(part(g, BIT[o] + BIT[p], THIRDS[d]), part(g, XYZ, THIRDS[d]), g, 9 + d, peers[d])

    def to_core(g, k, v, src=None):
        return copy(place(g, v, 0) if src is None else src, place(g, v, 1), g, 12 + k, peers[3])

    core_places = [0] + [BIT[d] for d in range(3)] + [BIT[a] + BIT[b] for a, b in PAIRS] + [XYZ]

    def stage0(g):
        @pl.when(g < S)
        def _():
            src, _ = own(g)
            for d in range(3):
                to_axis(g, d, src).start()
            to_core(g, 0, 0, src).start()

        @pl.when(g >= S)
        def _():
            _, src = own(g)
            for d in range(3):
                to_axis(g, d, src).start()
            to_core(g, 0, 0, src).start()

    def stage1(g):
        for d in range(3):
            to_axis(g, d, place(g, 0, 0)).wait_recv()
        for q in range(3):
            for h in range(2):
                relay(g, q, h).start()
        for d in range(3):
            to_core(g, 1 + d, BIT[d]).start()

    def stage2(g):
        for q in range(3):
            for h in range(2):
                relay(g, q, h).wait_recv()
        for d in range(3):
            relay_last(g, d).start()
        for q in range(3):
            to_core(g, 4 + q, core_places[4 + q]).start()

    def loads(g, slot):
        rest = pltpu.make_async_copy(buf.at[g, pl.ds(R, CHUNK - R)], rows_v.at[slot, pl.ds(R, CHUNK - R)], load_sem.at[slot, 0])
        mine = [pltpu.make_async_copy(src, rows_v.at[slot, pl.ds(0, R)], load_sem.at[slot, 1]) for src in own(g)]
        return rest, mine

    def act_loads(c, slot):
        for core in range(2):
            for v in range(8):
                j = me
                for d in range(3):
                    if v & BIT[d]:
                        j = flip(j, MASKS[d])
                if core:
                    j = flip(j, 1)
                at = pl.multiple_of(j * (S * R) + c * R, R)
                to = pl.ds((core * 8 + v) * R, R)
                pltpu.make_async_copy(gate.at[pl.ds(at, R)], gate_v.at[slot, to], act_sem.at[slot, 0]).start()
                pltpu.make_async_copy(up.at[pl.ds(at, R)], up_v.at[slot, to], act_sem.at[slot, 1]).start()

    def act_wait(slot):
        pltpu.make_async_copy(gate.at[pl.ds(0, CHUNK)], gate_v.at[slot], act_sem.at[slot, 0]).wait()
        pltpu.make_async_copy(up.at[pl.ds(0, CHUNK)], up_v.at[slot], act_sem.at[slot, 1]).wait()

    def dgu_load(c, slot):
        return pltpu.make_async_copy(dgu.at[c], dgu_v.at[slot], act_sem.at[slot, 0])

    def dgu_store(c, slot):
        return pltpu.make_async_copy(dgu_v.at[slot], dgu.at[c], put_sem.at[slot])

    def stage3(g):
        for d in range(3):
            relay_last(g, d).wait_recv()
        to_core(g, 7, XYZ).start()
        for k, v in enumerate(core_places):
            to_core(g, k, v).wait_recv()
        slot = g % 2
        rest, mine = loads(g, slot)
        rest.start()

        @pl.when(g < S)
        def _():
            mine[0].start()
            act_loads(g, slot)

        @pl.when(g >= S)
        def _():
            mine[1].start()

            @pl.when(g >= S + 2)
            def _():
                dgu_load(g - S, slot).start()

    def drain(g):
        for d in range(3):
            to_axis(g, d, place(g, 0, 0)).wait_send()
            relay_last(g, d).wait_send()
        for q in range(3):
            for h in range(2):
                relay(g, q, h).wait_send()
        for k, v in enumerate(core_places):
            to_core(g, k, v).wait_send()

    def act_tile(slot, t):
        rows = pl.ds(t * 256, 256)
        d_hidden = lax.dot_general(rows_v[slot, rows, :], wd_v[...], (((1,), (1,)), ((), ())), preferred_element_type=F32)
        hidden, back = jax.vjp(act, gate_v[slot, rows, :].astype(F32), up_v[slot, rows, :].astype(F32))
        d_gate, d_up = back(d_hidden)
        dgu_v[slot, rows, pl.ds(0, FL)] = d_gate.astype(BF)
        dgu_v[slot, rows, pl.ds(FL, FL)] = d_up.astype(BF)
        ht_v[:, rows] = hidden.T.astype(BF)

    def down_tile(slot, n):
        cols = pl.ds(pl.multiple_of(n * FL, 128), FL)
        rows, to = pl.ds(pl.multiple_of((n // 2) * FL, FL), FL), pl.ds(pl.multiple_of((n % 2) * FL, FL), FL)
        acc[rows, to] += jnp.dot(ht_v[...], rows_v[slot, :, cols], preferred_element_type=F32)

    def put_down():
        copies = []
        for i in range(14):
            r, c = i % 7, i // 7
            if i >= 2:
                copies[i - 2].wait()
            rows, cols = pl.ds(r * 128, 128), pl.ds(c * 1792, 1792)
            stage[i % 2, pl.ds(0, 128), :] = acc[pl.ds(i * 128, 128), :].astype(BF)
            copies.append(pltpu.make_async_copy(stage.at[i % 2, pl.ds(0, 128)], dw_down.at[rows, cols], out_sem.at[i % 2, 0]))
            copies[i].start()
        copies[12].wait()
        copies[13].wait()
        acc[pl.ds(0, 2 * FL), :] = jnp.zeros((2 * FL, 2 * FL), F32)

    def put_gu(m, slot):
        rows = pl.ds(pl.multiple_of(m * 256, 256), 256)
        return (
            pltpu.make_async_copy(stage.at[slot, :, pl.ds(0, FL)], dw_gate.at[rows], out_sem.at[slot, 0]),
            pltpu.make_async_copy(stage.at[slot, :, pl.ds(FL, FL)], dw_up.at[rows], out_sem.at[slot, 1]),
        )

    def gu_tile(g, slot, m):
        rows = pl.ds(pl.multiple_of(m * 256, 256), 256)
        acc[rows, :] += lax.dot_general(rows_v[slot, :, rows], dgu_v[slot], (((0,), (0,)), ((), ())), preferred_element_type=F32)

        @pl.when(g == last - 1)
        def _():
            at = m % 2

            @pl.when(m >= 2)
            def _():
                for c in put_gu(m - 2, at):
                    c.wait()

            stage[at] = acc[rows, :].astype(BF)
            for c in put_gu(m, at):
                c.start()

    def compute_first(g):
        slot = g % 2

        @pl.when(g < S)
        def _():
            rest, mine = loads(g, slot)
            rest.wait()
            mine[0].wait()
            act_wait(slot)

            @pl.when(g >= 2)
            def _():
                dgu_store(g - 2, slot).wait()

            act_tile(slot, 0)

        @pl.when(g >= S)
        def _():
            rest, mine = loads(g, slot)
            rest.wait()
            mine[1].wait()

            @pl.when(g < S + 2)
            def _():
                dgu_store(g - 2, slot).wait()
                dgu_load(g - S, slot).start()

            dgu_load(g - S, slot).wait()

            @pl.loop(0, 7)
            def _(m):
                gu_tile(g, slot, m)

    def compute_second(g):
        slot = g % 2

        @pl.when(g < S)
        def _():
            act_tile(slot, 1)
            dgu_store(g, slot).start()

            @pl.loop(0, 4)
            def _(n):
                down_tile(slot, n)

            @pl.when(g == S - 1)
            def _():
                put_down()

        @pl.when(g >= S)
        def _():
            @pl.loop(7, 14)
            def _(m):
                gu_tile(g, slot, m)

    weights = pltpu.make_async_copy(w_down, wd_v, w_sem)
    weights.start()
    greet(peers)
    stage0(jnp.int32(0))
    stage0(jnp.int32(1))
    acc[...] = jnp.zeros_like(acc)
    weights.wait()

    @pl.loop(0, last + 3)
    def _(i):
        @pl.when(i < last)
        def _():
            stage1(i)

        @pl.when(i + 2 < last)
        def _():
            @pl.when(i + 2 >= RING)
            def _():
                drain(i + 2 - RING)

            stage0(i + 2)

        @pl.when(i >= 3)
        def _():
            compute_first(i - 3)

        @pl.when(jnp.logical_and(i >= 1, i < last + 1))
        def _():
            stage2(i - 1)

        @pl.when(i >= 3)
        def _():
            compute_second(i - 3)

        @pl.when(jnp.logical_and(i >= 2, i < last + 2))
        def _():
            stage3(i - 2)

    @pl.loop(last - RING, last)
    def _(g):
        drain(g)

    for m in (12, 13):
        for c in put_gu(m, m % 2):
            c.wait()


def scatter_kernel(dgu, w_gate, w_up, dx,
                   w_v, dgu_v, part_v, core_s, core_r, s3, r3, s2, r2, s1, r1, out_v,
                   ss, rs, load_sem, w_sem, out_sem):
    me = lax.axis_index("tp")
    peers = peers_of(me)
    ring = 4

    def copy(src, dst, g, k, peer):
        return send(src, dst, ss.at[g % ring, k], rs.at[g % ring, k], peer)

    def to_core(g):
        return copy(core_s.at[g % 2], core_r.at[g % 2], g, 0, peers[3])

    def third(g, d):
        cols = pl.ds(*THIRDS[d])
        return copy(s3.at[g % 2, :, cols], r3.at[g % ring, :, cols], g, 1 + d, peers[d])

    def second(g, q, h):
        cols = pl.ds(*HALVES[h])
        return copy(s2.at[g % 2, q, :, cols], r2.at[g % ring, q, :, cols], g, 4 + 2 * q + h, peers[PAIRS[q][h]])

    def first(g, d):
        return copy(s1.at[g % 2, d], r1.at[g % ring, d], g, 10 + d, peers[d])

    def rows(v):
        return pl.ds(v * R, R)

    def load(g):
        return pltpu.make_async_copy(dgu.at[g], dgu_v.at[g % 2], load_sem.at[g % 2])

    def put(g):
        return pltpu.make_async_copy(out_v.at[g % 2], dx.at[pl.ds(pl.multiple_of(g * R, R), R)], out_sem.at[g % 2])

    def before(g, waits):
        @pl.when(g >= 2)
        def _():
            for c in waits(g - 2):
                c.wait_send()

    def thirds(g):
        return [third(g, d) for d in range(3)]

    def seconds(g):
        return [second(g, q, h) for q in range(3) for h in range(2)]

    def firsts(g):
        return [first(g, d) for d in range(3)]

    def multiply(g):
        slot = g % 2
        load(g).wait()

        @pl.when(g + 1 < S)
        def _():
            load(g + 1).start()

        before(g, lambda h: [to_core(h)])

        @pl.loop(0, 7)
        def _(n):
            cols = pl.ds(pl.multiple_of(n * 512, 512), 512)
            product = lax.dot_general(dgu_v[slot], w_v[cols, :], (((1,), (1,)), ((), ())), preferred_element_type=F32)
            part_v[g % 5, :, cols] = product[:HALF]
            core_s[slot, :, cols] = product[HALF:].astype(BF)

        to_core(g).start()

    def add_core(g):
        to_core(g).wait_recv()
        before(g, thirds)
        at = g % 5
        s3[g % 2] = (part_v[at, rows(XYZ), :] + core_r[g % 2, rows(XYZ), :].astype(F32)).astype(BF)
        low = pl.ds(0, XYZ * R)
        part_v[at, low, :] = part_v[at, low, :] + core_r[g % 2, low, :].astype(F32)
        for c in thirds(g):
            c.start()

    def add_thirds(g):
        for c in thirds(g):
            c.wait_recv()
        before(g, seconds)
        at = g % 5
        for q, (a, b) in enumerate(PAIRS):
            d = 3 - a - b
            v = BIT[a] + BIT[b]
            for e in range(3):
                cols = pl.ds(*THIRDS[e])
                value = part_v[at, rows(v), cols]
                if e == d:
                    value = value + r3[g % ring, :, cols].astype(F32)
                s2[g % 2, q, :, cols] = value.astype(BF)
        for c in seconds(g):
            c.start()

    def add_seconds(g):
        for c in seconds(g):
            c.wait_recv()
        before(g, firsts)
        at = g % 5
        for q, (a, b) in enumerate(PAIRS):
            for h, d in ((0, b), (1, a)):
                cols = pl.ds(*HALVES[h])
                s1[g % 2, d, :, cols] = (part_v[at, rows(BIT[d]), cols] + r2[g % ring, q, :, cols].astype(F32)).astype(BF)
        for c in firsts(g):
            c.start()

    def add_firsts(g):
        for c in firsts(g):
            c.wait_recv()

        @pl.when(g >= 2)
        def _():
            put(g - 2).wait()

        total = part_v[g % 5, rows(0), :]
        for d in range(3):
            total = total + r1[g % ring, d].astype(F32)
        out_v[g % 2] = total.astype(BF)
        put(g).start()

    w_copies = [
        pltpu.make_async_copy(w_gate, w_v.at[:, pl.ds(0, FL)], w_sem.at[0]),
        pltpu.make_async_copy(w_up, w_v.at[:, pl.ds(FL, FL)], w_sem.at[1]),
    ]
    for c in w_copies:
        c.start()
    load(jnp.int32(0)).start()
    greet(peers)
    for c in w_copies:
        c.wait()

    @pl.loop(0, S + 4)
    def _(i):
        for lag, step in ((2, add_thirds), (3, add_seconds), (4, add_firsts), (1, add_core)):
            @pl.when(jnp.logical_and(i >= lag, i < S + lag))
            def _(lag=lag, step=step):
                step(i - lag)

        @pl.when(i < S)
        def _():
            multiply(i)

    for g in (S - 2, S - 1):
        g = jnp.int32(g)
        for c in [to_core(g), *thirds(g), *seconds(g), *firsts(g)]:
            c.wait_send()
        put(g).wait()


def solution(mesh):
    any_space = pl.BlockSpec(memory_space=pl.ANY)
    dma = pltpu.SemaphoreType.DMA

    def body(x, dy, gate, up, w_gate, w_up, w_down):
        dgu, dw_gate, dw_up, dw_down, _ = pl.pallas_call(
            gather_kernel,
            out_shape=[
                jax.ShapeDtypeStruct((S, CHUNK, 2 * FL), BF),
                jax.ShapeDtypeStruct((D, FL), BF),
                jax.ShapeDtypeStruct((D, FL), BF),
                jax.ShapeDtypeStruct((FL, D), BF),
                jax.ShapeDtypeStruct((2 * S, CHUNK, D), BF),
            ],
            in_specs=[any_space] * 5,
            out_specs=[any_space] * 5,
            scratch_shapes=[
                pltpu.VMEM((FL, D), BF),
                pltpu.VMEM((D, 2 * FL), F32),
                pltpu.VMEM((2, CHUNK, D), BF),
                pltpu.VMEM((2, CHUNK, FL), BF),
                pltpu.VMEM((2, CHUNK, FL), BF),
                pltpu.VMEM((2, CHUNK, 2 * FL), BF),
                pltpu.VMEM((FL, CHUNK), BF),
                pltpu.VMEM((2, 256, 2 * FL), BF),
                dma((RING, 20)),
                dma((RING, 20)),
                dma((2, 2)),
                dma((2, 2)),
                dma,
                dma((2,)),
                dma((2, 2)),
            ],
            compiler_params=pltpu.CompilerParams(collective_id=0, has_side_effects=True, vmem_limit_bytes=VMEM_LIMIT),
            name="gather_dy_x",
        )(dy, x, gate, up, w_down)
        dx = pl.pallas_call(
            scatter_kernel,
            out_shape=jax.ShapeDtypeStruct((S * R, D), BF),
            in_specs=[any_space] * 3,
            out_specs=any_space,
            scratch_shapes=[
                pltpu.VMEM((D, 2 * FL), BF),
                pltpu.VMEM((2, CHUNK, 2 * FL), BF),
                pltpu.VMEM((5, HALF, D), F32),
                pltpu.VMEM((2, HALF, D), BF),
                pltpu.VMEM((2, HALF, D), BF),
                pltpu.VMEM((2, R, D), BF),
                pltpu.VMEM((4, R, D), BF),
                pltpu.VMEM((2, 3, R, D), BF),
                pltpu.VMEM((4, 3, R, D), BF),
                pltpu.VMEM((2, 3, R, D), BF),
                pltpu.VMEM((4, 3, R, D), BF),
                pltpu.VMEM((2, R, D), BF),
                dma((4, 13)),
                dma((4, 13)),
                dma((2,)),
                dma((2,)),
                dma((2,)),
            ],
            compiler_params=pltpu.CompilerParams(collective_id=1, has_side_effects=True, vmem_limit_bytes=VMEM_LIMIT),
            name="scatter_dx",
        )(dgu, w_gate, w_up)
        return dx, dw_gate, dw_up, dw_down

    rows, cols = P(("dp", "tp"), None), P("dp", "tp")
    return jax.shard_map(
        body,
        mesh=mesh,
        in_specs=(rows, rows, cols, cols, P(None, "tp"), P(None, "tp"), P("tp", None)),
        out_specs=(rows, cols, cols, rows),
        check_vma=False,
    )
```

```python
import functools

import jax
import jax.numpy as jnp
from jax import lax
from jax.experimental import pallas as pl
from jax.experimental.pallas import tpu as pltpu
from jax.sharding import PartitionSpec as P

BF = jnp.bfloat16
F32 = jnp.float32
S = 10
R = 32
RING = 8
CHUNK = 16 * R
HALF = 8 * R
D = 3584
FL = 896
MASKS = (8, 4, 2)
BIT = (4, 2, 1)
HALVES = ((0, 1792), (1792, 1792))
THIRDS = ((0, 1152), (1152, 1280), (2432, 1152))
PAIRS = ((0, 1), (1, 2), (2, 0))
OTHERS = ((1, 2), (0, 2), (0, 1))
XYZ = 7
TA = 512
TM = 256
NM = 8
NB = D // TM - NM
UG = 4
VMEM_LIMIT = 67_000_000


def act(gate, up):
    return jax.nn.gelu(gate) * up


def flip(me, mask):
    return me + mask * (1 - 2 * ((me // mask) % 2))


def peers_of(me):
    return [flip(me, m) for m in MASKS] + [flip(me, 1)]


def greet(peers):
    barrier = pltpu.get_barrier_semaphore()
    for peer in peers:
        pl.semaphore_signal(barrier, inc=1, device_id={"tp": peer}, device_id_type=pl.DeviceIdType.MESH)
    pl.semaphore_wait(barrier, len(peers))


def send(src, dst, send_sem, recv_sem, peer):
    return pltpu.make_async_remote_copy(
        src_ref=src, dst_ref=dst, send_sem=send_sem, recv_sem=recv_sem,
        device_id={"tp": peer}, device_id_type=pl.DeviceIdType.MESH,
    )


def gather_kernel(dy, x, gate, up, w_down, dgu, dw_gate, dw_up, dw_down, buf,
                  wd_v, acc, rows_v, gate_v, up_v, dgu_v, ht_v, stage,
                  ss, rs, load_sem, act_sem, w_sem, put_sem, out_sem):
    me = lax.axis_index("tp")
    peers = peers_of(me)
    last = 2 * S

    def place(g, v, core):
        return buf.at[g, pl.ds((core * 8 + v) * R, R)]

    def part(g, v, cols):
        return buf.at[g, pl.ds(v * R, R), pl.ds(*cols)]

    def own(g):
        return dy.at[pl.ds(g * R, R)], x.at[pl.ds((g - S) * R, R)]

    def copy(src, dst, g, k, peer):
        return send(src, dst, ss.at[g % RING, k], rs.at[g % RING, k], peer)

    def to_axis(g, d, src):
        return copy(src, place(g, BIT[d], 0), g, d, peers[d])

    def relay(g, q, h):
        a, b = PAIRS[q]
        via, src = (a, b) if h == 0 else (b, a)
        return copy(part(g, BIT[src], HALVES[h]), part(g, BIT[a] + BIT[b], HALVES[h]), g, 3 + 2 * q + h, peers[via])

    def relay_last(g, d):
        o, p = OTHERS[d]
        return copy(part(g, BIT[o] + BIT[p], THIRDS[d]), part(g, XYZ, THIRDS[d]), g, 9 + d, peers[d])

    def to_core(g, k, v, src=None):
        return copy(place(g, v, 0) if src is None else src, place(g, v, 1), g, 12 + k, peers[3])

    core_places = [0] + [BIT[d] for d in range(3)] + [BIT[a] + BIT[b] for a, b in PAIRS] + [XYZ]

    def stage0(g):
        @pl.when(g < S)
        def _():
            src, _ = own(g)
            for d in range(3):
                to_axis(g, d, src).start()
            to_core(g, 0, 0, src).start()

        @pl.when(g >= S)
        def _():
            _, src = own(g)
            for d in range(3):
                to_axis(g, d, src).start()
            to_core(g, 0, 0, src).start()

    def stage1(g):
        for d in range(3):
            to_axis(g, d, place(g, 0, 0)).wait_recv()
        for q in range(3):
            for h in range(2):
                relay(g, q, h).start()
        for d in range(3):
            to_core(g, 1 + d, BIT[d]).start()

    def stage2(g):
        for q in range(3):
            for h in range(2):
                relay(g, q, h).wait_recv()
        for d in range(3):
            relay_last(g, d).start()
        for q in range(3):
            to_core(g, 4 + q, core_places[4 + q]).start()

    def loads(g, slot):
        rest = pltpu.make_async_copy(buf.at[g, pl.ds(R, CHUNK - R)], rows_v.at[slot, pl.ds(R, CHUNK - R)], load_sem.at[slot, 0])
        mine = [pltpu.make_async_copy(src, rows_v.at[slot, pl.ds(0, R)], load_sem.at[slot, 1]) for src in own(g)]
        return rest, mine

    def act_loads(c, slot):
        for core in range(2):
            for v in range(8):
                j = me
                for d in range(3):
                    if v & BIT[d]:
                        j = flip(j, MASKS[d])
                if core:
                    j = flip(j, 1)
                at = pl.multiple_of(j * (S * R) + c * R, R)
                to = pl.ds((core * 8 + v) * R, R)
                pltpu.make_async_copy(gate.at[pl.ds(at, R)], gate_v.at[slot, to], act_sem.at[slot, 0]).start()
                pltpu.make_async_copy(up.at[pl.ds(at, R)], up_v.at[slot, to], act_sem.at[slot, 1]).start()

    def act_wait(slot):
        pltpu.make_async_copy(gate.at[pl.ds(0, CHUNK)], gate_v.at[slot], act_sem.at[slot, 0]).wait()
        pltpu.make_async_copy(up.at[pl.ds(0, CHUNK)], up_v.at[slot], act_sem.at[slot, 1]).wait()

    def dgu_load(c, slot):
        return pltpu.make_async_copy(dgu.at[c], dgu_v.at[slot], act_sem.at[slot, 0])

    def dgu_store(c, slot):
        return pltpu.make_async_copy(dgu_v.at[slot], dgu.at[c], put_sem.at[slot])

    def stage3(g):
        for d in range(3):
            relay_last(g, d).wait_recv()
        to_core(g, 7, XYZ).start()
        for k, v in enumerate(core_places):
            to_core(g, k, v).wait_recv()
        slot = g % 2
        rest, mine = loads(g, slot)
        rest.start()

        @pl.when(g < S)
        def _():
            mine[0].start()
            act_loads(g, slot)

        @pl.when(g >= S)
        def _():
            mine[1].start()

            @pl.when(g >= S + 2)
            def _():
                dgu_load(g - S, slot).start()

    def drain(g):
        for d in range(3):
            to_axis(g, d, place(g, 0, 0)).wait_send()
            relay_last(g, d).wait_send()
        for q in range(3):
            for h in range(2):
                relay(g, q, h).wait_send()
        for k, v in enumerate(core_places):
            to_core(g, k, v).wait_send()

    def act_tile(slot, t):
        rows = pl.ds(t * TA, TA)
        d_hidden = lax.dot_general(rows_v[slot, rows, :], wd_v[...], (((1,), (1,)), ((), ())), preferred_element_type=F32)
        hidden, back = jax.vjp(act, gate_v[slot, rows, :].astype(F32), up_v[slot, rows, :].astype(F32))
        d_gate, d_up = back(d_hidden)
        dgu_v[slot, rows, pl.ds(0, FL)] = d_gate.astype(BF)
        dgu_v[slot, rows, pl.ds(FL, FL)] = d_up.astype(BF)
        ht_v[:, rows] = hidden.T.astype(BF)

    def down_tile(slot, n):
        cols = pl.ds(pl.multiple_of(n * FL, 128), FL)
        rows, to = pl.ds(pl.multiple_of((n // 2) * FL, FL), FL), pl.ds(pl.multiple_of((n % 2) * FL, FL), FL)
        acc[rows, to] += jnp.dot(ht_v[...], rows_v[slot, :, cols], preferred_element_type=F32)

    def put_down():
        copies = []
        for i in range(14):
            r, c = i % 7, i // 7
            if i >= 2:
                copies[i - 2].wait()
            rows, cols = pl.ds(r * 128, 128), pl.ds(c * 1792, 1792)
            stage[i % 2, pl.ds(0, 128), :] = acc[pl.ds(i * 128, 128), :].astype(BF)
            copies.append(pltpu.make_async_copy(stage.at[i % 2, pl.ds(0, 128)], dw_down.at[rows, cols], out_sem.at[i % 2, 0]))
            copies[i].start()
        copies[12].wait()
        copies[13].wait()
        acc[pl.ds(0, 2 * FL), :] = jnp.zeros((2 * FL, 2 * FL), F32)

    def put_gu(m, slot):
        rows = pl.ds(pl.multiple_of(m * TM, TM), TM)
        return (
            pltpu.make_async_copy(stage.at[slot, :, pl.ds(0, FL)], dw_gate.at[rows], out_sem.at[slot, 0]),
            pltpu.make_async_copy(stage.at[slot, :, pl.ds(FL, FL)], dw_up.at[rows], out_sem.at[slot, 1]),
        )

    def gu_tile(slot, m, flush):
        rows = pl.ds(pl.multiple_of(m * TM, TM), TM)
        total = acc[rows, :] + lax.dot_general(rows_v[slot, :, rows], dgu_v[slot], (((0,), (0,)), ((), ())), preferred_element_type=F32)
        if not flush:
            acc[rows, :] = total
            return
        at = m % 2

        @pl.when(m >= 2)
        def _():
            for c in put_gu(m - 2, at):
                c.wait()

        stage[at] = total.astype(BF)
        for c in put_gu(m, at):
            c.start()

    def gu_tiles(g, slot, low, high):
        @pl.when(g < last - 1)
        def _():
            @pl.loop(low, high, unroll=UG)
            def _(m):
                gu_tile(slot, m, False)

        @pl.when(g == last - 1)
        def _():
            @pl.loop(low, high)
            def _(m):
                gu_tile(slot, m, True)

    def compute_first(g):
        slot = g % 2

        @pl.when(g < S)
        def _():
            rest, mine = loads(g, slot)
            rest.wait()
            mine[0].wait()
            act_wait(slot)

            @pl.when(g >= 2)
            def _():
                dgu_store(g - 2, slot).wait()

            for t in range(CHUNK // TA // 2 + CHUNK // TA % 2):
                act_tile(slot, t)

        @pl.when(g >= S)
        def _():
            rest, mine = loads(g, slot)
            rest.wait()
            mine[1].wait()

            @pl.when(g < S + 2)
            def _():
                dgu_store(g - 2, slot).wait()
                dgu_load(g - S, slot).start()

            dgu_load(g - S, slot).wait()

            gu_tiles(g, slot, 0, NM // 2)

    def compute_second(g):
        slot = g % 2

        @pl.when(g < S)
        def _():
            for t in range(CHUNK // TA // 2 + CHUNK // TA % 2, CHUNK // TA):
                act_tile(slot, t)
            dgu_store(g, slot).start()

            @pl.loop(0, 4)
            def _(n):
                down_tile(slot, n)

            @pl.when(g == S - 1)
            def _():
                put_down()

        @pl.when(g >= S)
        def _():
            gu_tiles(g, slot, NM // 2, NM)

    weights = pltpu.make_async_copy(w_down, wd_v, w_sem)
    weights.start()
    greet(peers)
    stage0(jnp.int32(0))
    stage0(jnp.int32(1))
    acc[...] = jnp.zeros_like(acc)
    weights.wait()

    @pl.loop(0, last + 4)
    def _(i):
        @pl.when(i < last)
        def _():
            stage1(i)

        @pl.when(i + 2 < last)
        def _():
            @pl.when(i + 2 >= RING)
            def _():
                drain(i + 2 - RING)

            stage0(i + 2)

        @pl.when(jnp.logical_and(i >= 3, i < last + 3))
        def _():
            stage3(i - 3)

        @pl.when(i >= 4)
        def _():
            compute_first(i - 4)

        @pl.when(jnp.logical_and(i >= 1, i < last + 1))
        def _():
            stage2(i - 1)

        @pl.when(i >= 4)
        def _():
            compute_second(i - 4)

    @pl.loop(last - RING, last)
    def _(g):
        drain(g)

    for m in (NM - 2, NM - 1):
        for c in put_gu(m, m % 2):
            c.wait()


def scatter_kernel(dgu, w_gate, w_up, x, buf, dw_gate_in, dw_up_in, dx, dw_gate, dw_up,
                   acc, x_v, w_v, dgu_v, part_v, sum2, sum1, sum0, core_s, core_r, s3, r3, s2, r2, s1, r1, out_v,
                   ss, rs, load_sem, x_sem, w_sem, out_sem, put_sem):
    me = lax.axis_index("tp")
    peers = peers_of(me)
    ring = 4
    x_cols = pl.ds(NM * TM, NB * TM)

    def copy(src, dst, g, k, peer):
        return send(src, dst, ss.at[g % ring, k], rs.at[g % ring, k], peer)

    def to_core(g):
        return copy(core_s.at[g % 2], core_r.at[g % 2], g, 0, peers[3])

    def third(g, d):
        cols = pl.ds(*THIRDS[d])
        return copy(s3.at[g % 2, :, cols], r3.at[g % ring, :, cols], g, 1 + d, peers[d])

    def second(g, q, h):
        cols = pl.ds(*HALVES[h])
        return copy(s2.at[g % 2, q, :, cols], r2.at[g % ring, q, :, cols], g, 4 + 2 * q + h, peers[PAIRS[q][h]])

    def first(g, d):
        return copy(s1.at[g % 2, d], r1.at[g % ring, d], g, 10 + d, peers[d])

    def rows(v):
        return pl.ds(v * R, R)

    def load(g):
        at = g % 2
        return (
            pltpu.make_async_copy(dgu.at[g], dgu_v.at[at], load_sem.at[at]),
            pltpu.make_async_copy(x.at[pl.ds(pl.multiple_of(g * R, R), R), x_cols], x_v.at[at, pl.ds(0, R)], x_sem.at[at, 0]),
            pltpu.make_async_copy(buf.at[S + g, pl.ds(R, CHUNK - R), x_cols], x_v.at[at, pl.ds(R, CHUNK - R)], x_sem.at[at, 1]),
        )

    def put_gu(m):
        rows, src = pl.ds((NM + m) * TM, TM), w_v.at[pl.ds(m * TM, TM)]
        return (
            pltpu.make_async_copy(src.at[:, pl.ds(0, FL)], dw_gate.at[rows], put_sem.at[m, 0]),
            pltpu.make_async_copy(src.at[:, pl.ds(FL, FL)], dw_up.at[rows], put_sem.at[m, 1]),
        )

    def put(g):
        return pltpu.make_async_copy(out_v.at[g % 2], dx.at[pl.ds(pl.multiple_of(g * R, R), R)], out_sem.at[g % 2])

    def before(g, waits):
        @pl.when(g >= 2)
        def _():
            for c in waits(g - 2):
                c.wait_send()

    def thirds(g):
        return [third(g, d) for d in range(3)]

    def seconds(g):
        return [second(g, q, h) for q in range(3) for h in range(2)]

    def firsts(g):
        return [first(g, d) for d in range(3)]

    def multiply(g):
        slot = g % 2
        for c in load(g):
            c.wait()

        @pl.when(g + 1 < S)
        def _():
            for c in load(g + 1):
                c.start()

        before(g, lambda h: [to_core(h)])

        @pl.loop(0, 7, unroll=7)
        def _(n):
            cols = pl.ds(pl.multiple_of(n * 512, 512), 512)
            product = lax.dot_general(dgu_v[slot], w_v[cols, :], (((1,), (1,)), ((), ())), preferred_element_type=F32)
            part_v[:, cols] = product[:HALF]
            core_s[slot, :, cols] = product[HALF:].astype(BF)

        to_core(g).start()
        for m in range(NB):
            rows = pl.ds(m * TM, TM)
            acc[rows, :] += lax.dot_general(x_v[slot, :, rows], dgu_v[slot], (((0,), (0,)), ((), ())), preferred_element_type=F32)

    def add_core(g):
        to_core(g).wait_recv()
        before(g, thirds)

        def both(v):
            return part_v[rows(v), :] + core_r[g % 2, rows(v), :].astype(F32)

        s3[g % 2] = both(XYZ).astype(BF)
        for q, (a, b) in enumerate(PAIRS):
            sum2[g % 2, q] = both(BIT[a] + BIT[b])
        for d in range(3):
            sum1[g % 3, d] = both(BIT[d])
        sum0[g % 4] = both(0)
        for c in thirds(g):
            c.start()

    def add_thirds(g):
        for c in thirds(g):
            c.wait_recv()
        before(g, seconds)
        for q, (a, b) in enumerate(PAIRS):
            d = 3 - a - b
            for e in range(3):
                cols = pl.ds(*THIRDS[e])
                value = sum2[g % 2, q, :, cols]
                if e == d:
                    value = value + r3[g % ring, :, cols].astype(F32)
                s2[g % 2, q, :, cols] = value.astype(BF)
        for c in seconds(g):
            c.start()

    def add_seconds(g):
        for c in seconds(g):
            c.wait_recv()
        before(g, firsts)
        for q, (a, b) in enumerate(PAIRS):
            for h, d in ((0, b), (1, a)):
                cols = pl.ds(*HALVES[h])
                s1[g % 2, d, :, cols] = (sum1[g % 3, d, :, cols] + r2[g % ring, q, :, cols].astype(F32)).astype(BF)
        for c in firsts(g):
            c.start()

    def add_firsts(g):
        for c in firsts(g):
            c.wait_recv()

        @pl.when(g >= 2)
        def _():
            put(g - 2).wait()

        total = sum0[g % 4]
        for d in range(3):
            total = total + r1[g % ring, d].astype(F32)
        out_v[g % 2] = total.astype(BF)
        put(g).start()

    w_copies = [
        pltpu.make_async_copy(w_gate, w_v.at[:, pl.ds(0, FL)], w_sem.at[0]),
        pltpu.make_async_copy(w_up, w_v.at[:, pl.ds(FL, FL)], w_sem.at[1]),
    ]
    for c in w_copies:
        c.start()
    for c in load(jnp.int32(0)):
        c.start()
    greet(peers)
    acc[...] = jnp.zeros_like(acc)
    for c in w_copies:
        c.wait()

    @pl.loop(0, S + 4)
    def _(i):
        for lag, step in ((1, add_core), (2, add_thirds), (3, add_seconds), (4, add_firsts)):
            @pl.when(jnp.logical_and(i >= lag, i < S + lag))
            def _(lag=lag, step=step):
                step(i - lag)

        @pl.when(i < S)
        def _():
            multiply(i)

        @pl.when(i == S)
        def _():
            for m in range(NB):
                w_v[pl.ds(m * TM, TM), :] = acc[pl.ds(m * TM, TM), :].astype(BF)
            for m in range(NB):
                for c in put_gu(m):
                    c.start()

    for g in (S - 2, S - 1):
        g = jnp.int32(g)
        for c in [to_core(g), *thirds(g), *seconds(g), *firsts(g)]:
            c.wait_send()
        put(g).wait()
    for m in range(NB):
        for c in put_gu(m):
            c.wait()


def solution(mesh):
    any_space = pl.BlockSpec(memory_space=pl.ANY)
    dma = pltpu.SemaphoreType.DMA

    def body(x, dy, gate, up, w_gate, w_up, w_down):
        dgu, dw_gate, dw_up, dw_down, buf = pl.pallas_call(
            gather_kernel,
            out_shape=[
                jax.ShapeDtypeStruct((S, CHUNK, 2 * FL), BF),
                jax.ShapeDtypeStruct((D, FL), BF),
                jax.ShapeDtypeStruct((D, FL), BF),
                jax.ShapeDtypeStruct((FL, D), BF),
                jax.ShapeDtypeStruct((2 * S, CHUNK, D), BF),
            ],
            in_specs=[any_space] * 5,
            out_specs=[any_space] * 5,
            scratch_shapes=[
                pltpu.VMEM((FL, D), BF),
                pltpu.VMEM((NM * TM, 2 * FL), F32),
                pltpu.VMEM((2, CHUNK, D), BF),
                pltpu.VMEM((2, CHUNK, FL), BF),
                pltpu.VMEM((2, CHUNK, FL), BF),
                pltpu.VMEM((2, CHUNK, 2 * FL), BF),
                pltpu.VMEM((FL, CHUNK), BF),
                pltpu.VMEM((2, TM, 2 * FL), BF),
                dma((RING, 20)),
                dma((RING, 20)),
                dma((2, 2)),
                dma((2, 2)),
                dma,
                dma((2,)),
                dma((2, 2)),
            ],
            compiler_params=pltpu.CompilerParams(collective_id=0, has_side_effects=True, vmem_limit_bytes=VMEM_LIMIT),
            name="gather_dy_x",
        )(dy, x, gate, up, w_down)
        dx, dw_gate, dw_up = pl.pallas_call(
            scatter_kernel,
            out_shape=[
                jax.ShapeDtypeStruct((S * R, D), BF),
                jax.ShapeDtypeStruct((D, FL), BF),
                jax.ShapeDtypeStruct((D, FL), BF),
            ],
            in_specs=[any_space] * 7,
            input_output_aliases={5: 1, 6: 2},
            out_specs=[any_space] * 3,
            scratch_shapes=[
                pltpu.VMEM((NB * TM, 2 * FL), F32),
                pltpu.VMEM((2, CHUNK, NB * TM), BF),
                pltpu.VMEM((D, 2 * FL), BF),
                pltpu.VMEM((2, CHUNK, 2 * FL), BF),
                pltpu.VMEM((HALF, D), F32),
                pltpu.VMEM((2, 3, R, D), F32),
                pltpu.VMEM((3, 3, R, D), F32),
                pltpu.VMEM((4, R, D), F32),
                pltpu.VMEM((2, HALF, D), BF),
                pltpu.VMEM((2, HALF, D), BF),
                pltpu.VMEM((2, R, D), BF),
                pltpu.VMEM((4, R, D), BF),
                pltpu.VMEM((2, 3, R, D), BF),
                pltpu.VMEM((4, 3, R, D), BF),
                pltpu.VMEM((2, 3, R, D), BF),
                pltpu.VMEM((4, 3, R, D), BF),
                pltpu.VMEM((2, R, D), BF),
                dma((4, 13)),
                dma((4, 13)),
                dma((2,)),
                dma((2, 2)),
                dma((2,)),
                dma((2,)),
                dma((NB, 2)),
            ],
            compiler_params=pltpu.CompilerParams(collective_id=1, has_side_effects=True, vmem_limit_bytes=VMEM_LIMIT),
            name="scatter_dx",
        )(dgu, w_gate, w_up, x, buf, dw_gate, dw_up)
        return dx, dw_gate, dw_up, dw_down

    rows, cols = P(("dp", "tp"), None), P("dp", "tp")
    return jax.shard_map(
        body,
        mesh=mesh,
        in_specs=(rows, rows, cols, cols, P(None, "tp"), P(None, "tp"), P("tp", None)),
        out_specs=(rows, cols, cols, rows),
        check_vma=False,
    )
```

```python
import functools

import jax
import jax.numpy as jnp
from jax import lax
from jax.experimental import pallas as pl
from jax.experimental.pallas import tpu as pltpu
from jax.sharding import PartitionSpec as P

BF = jnp.bfloat16
F32 = jnp.float32
S = 10
R = 32
RING = 8
CHUNK = 16 * R
HALF = 8 * R
D = 3584
FL = 896
MASKS = (8, 4, 2)
BIT = (4, 2, 1)
HALVES = ((0, 1792), (1792, 1792))
THIRDS = ((0, 1152), (1152, 1280), (2432, 1152))
PAIRS = ((0, 1), (1, 2), (2, 0))
OTHERS = ((1, 2), (0, 2), (0, 1))
XYZ = 7
TA = 512
TM = 256
NM = 8
NB = D // TM - NM
UG = 4
LAG = 3
X_STEPS = (((0, 0), (0, 1)), ((0, 2), (1, 0), (1, 1)), ((1, 2), (2, 0)), ((2, 1), (2, 2)))
FT = 512
XD = 3
VMEM_LIMIT = 67_000_000


def act(gate, up):
    return jax.nn.gelu(gate) * up


def flip(me, mask):
    return me + mask * (1 - 2 * ((me // mask) % 2))


def peers_of(me):
    return [flip(me, m) for m in MASKS] + [flip(me, 1)]


def greet(peers):
    barrier = pltpu.get_barrier_semaphore()
    for peer in peers:
        pl.semaphore_signal(barrier, inc=1, device_id={"tp": peer}, device_id_type=pl.DeviceIdType.MESH)
    pl.semaphore_wait(barrier, len(peers))


def send(src, dst, send_sem, recv_sem, peer):
    return pltpu.make_async_remote_copy(
        src_ref=src, dst_ref=dst, send_sem=send_sem, recv_sem=recv_sem,
        device_id={"tp": peer}, device_id_type=pl.DeviceIdType.MESH,
    )


def gather_ops(buf, ss, rs, ring, peers):
    places = [0] + [BIT[d] for d in range(3)] + [BIT[a] + BIT[b] for a, b in PAIRS] + [XYZ]

    def place(g, v, core):
        return buf.at[g, pl.ds((core * 8 + v) * R, R)]

    def part(g, v, cols):
        return buf.at[g, pl.ds(v * R, R), pl.ds(*cols)]

    def copy(src, dst, g, k, peer):
        return send(src, dst, ss.at[g % ring, k], rs.at[g % ring, k], peer)

    def to_axis(g, d, src=None):
        return copy(place(g, 0, 0) if src is None else src, place(g, BIT[d], 0), g, d, peers[d])

    def relays(g):
        for q, (a, b) in enumerate(PAIRS):
            for h, via, src in ((0, a, b), (1, b, a)):
                yield copy(part(g, BIT[src], HALVES[h]), part(g, BIT[a] + BIT[b], HALVES[h]), g, 3 + 2 * q + h, peers[via])

    def relay_last(g, d):
        o, p = OTHERS[d]
        return copy(part(g, BIT[o] + BIT[p], THIRDS[d]), part(g, XYZ, THIRDS[d]), g, 9 + d, peers[d])

    def to_core(g, k, src=None):
        return copy(place(g, places[k], 0) if src is None else src, place(g, places[k], 1), g, 12 + k, peers[3])

    def start(g, src):
        for d in range(3):
            to_axis(g, d, src).start()
        to_core(g, 0, src).start()

    def stage1(g):
        for d in range(3):
            to_axis(g, d).wait_recv()
        for c in relays(g):
            c.start()
        for k in (1, 2, 3):
            to_core(g, k).start()

    def stage2(g):
        for c in relays(g):
            c.wait_recv()
        for d in range(3):
            relay_last(g, d).start()
        for k in (4, 5, 6):
            to_core(g, k).start()

    def arrive(g):
        for d in range(3):
            relay_last(g, d).wait_recv()
        to_core(g, 7).start()
        for k in range(8):
            to_core(g, k).wait_recv()

    def drain(g):
        for d in range(3):
            to_axis(g, d).wait_send()
            relay_last(g, d).wait_send()
        for c in relays(g):
            c.wait_send()
        for k in range(8):
            to_core(g, k).wait_send()

    return start, stage1, stage2, arrive, drain


def gather_kernel(dy, x, gate, up, w_down, dgu, dw_part, dw_down, buf,
                  wd_v, acc, rows_v, gate_v, up_v, dgu_v, ht_v, stage,
                  ss, rs, load_sem, act_sem, w_sem, put_sem, out_sem):
    me = lax.axis_index("tp")
    peers = peers_of(me)
    last = 2 * S - XD
    start, stage1, stage2, arrive, drain = gather_ops(buf, ss, rs, RING, peers)

    def own(g):
        return dy.at[pl.ds(g * R, R)], x.at[pl.ds((g - S) * R, R)]

    def stage0(g):
        @pl.when(g < S)
        def _():
            start(g, own(g)[0])

        @pl.when(g >= S)
        def _():
            start(g, own(g)[1])

    def loads(g, slot):
        rest = pltpu.make_async_copy(buf.at[g, pl.ds(R, CHUNK - R)], rows_v.at[slot, pl.ds(R, CHUNK - R)], load_sem.at[slot, 0])
        mine = [pltpu.make_async_copy(src, rows_v.at[slot, pl.ds(0, R)], load_sem.at[slot, 1]) for src in own(g)]
        return rest, mine

    def act_loads(c, slot):
        for core in range(2):
            for v in range(8):
                j = me
                for d in range(3):
                    if v & BIT[d]:
                        j = flip(j, MASKS[d])
                if core:
                    j = flip(j, 1)
                at = pl.multiple_of(j * (S * R) + c * R, R)
                to = pl.ds((core * 8 + v) * R, R)
                pltpu.make_async_copy(gate.at[pl.ds(at, R)], gate_v.at[slot, to], act_sem.at[slot, 0]).start()
                pltpu.make_async_copy(up.at[pl.ds(at, R)], up_v.at[slot, to], act_sem.at[slot, 1]).start()

    def act_wait(slot):
        pltpu.make_async_copy(gate.at[pl.ds(0, CHUNK)], gate_v.at[slot], act_sem.at[slot, 0]).wait()
        pltpu.make_async_copy(up.at[pl.ds(0, CHUNK)], up_v.at[slot], act_sem.at[slot, 1]).wait()

    def dgu_load(c, slot):
        return pltpu.make_async_copy(dgu.at[c], dgu_v.at[slot], act_sem.at[slot, 0])

    def dgu_store(c, slot):
        return pltpu.make_async_copy(dgu_v.at[slot], dgu.at[c], put_sem.at[slot])

    def stage3(g):
        arrive(g)
        slot = g % 2
        rest, mine = loads(g, slot)
        rest.start()

        @pl.when(g < S)
        def _():
            mine[0].start()
            act_loads(g, slot)

        @pl.when(g >= S)
        def _():
            mine[1].start()

            @pl.when(g >= S + 2)
            def _():
                dgu_load(g - S, slot).start()

    def act_tile(slot, t):
        rows = pl.ds(t * TA, TA)
        d_hidden = lax.dot_general(rows_v[slot, rows, :], wd_v[...], (((1,), (1,)), ((), ())), preferred_element_type=F32)
        hidden, back = jax.vjp(act, gate_v[slot, rows, :].astype(F32), up_v[slot, rows, :].astype(F32))
        d_gate, d_up = back(d_hidden)
        dgu_v[slot, rows, pl.ds(0, FL)] = d_gate.astype(BF)
        dgu_v[slot, rows, pl.ds(FL, FL)] = d_up.astype(BF)
        ht_v[:, rows] = hidden.T.astype(BF)

    def down_tile(slot, n):
        cols = pl.ds(pl.multiple_of(n * FL, 128), FL)
        rows, to = pl.ds(pl.multiple_of((n // 2) * FL, FL), FL), pl.ds(pl.multiple_of((n % 2) * FL, FL), FL)
        acc[rows, to] += jnp.dot(ht_v[...], rows_v[slot, :, cols], preferred_element_type=F32)

    def put_down():
        copies = []
        for i in range(14):
            r, c = i % 7, i // 7
            if i >= 2:
                copies[i - 2].wait()
            rows, cols = pl.ds(r * 128, 128), pl.ds(c * 1792, 1792)
            stage[i % 2, pl.ds(0, 128), :] = acc[pl.ds(i * 128, 128), :].astype(BF)
            copies.append(pltpu.make_async_copy(stage.at[i % 2, pl.ds(0, 128)], dw_down.at[rows, cols], out_sem.at[i % 2, 0]))
            copies[i].start()
        copies[12].wait()
        copies[13].wait()
        acc[pl.ds(0, 2 * FL), :] = jnp.zeros((2 * FL, 2 * FL), F32)

    def put_gu(half):
        rows = pl.ds(half * (NM // 2 * TM), NM // 2 * TM)
        return pltpu.make_async_copy(acc.at[rows], dw_part.at[rows], out_sem.at[half, 1])

    def gu_tile(slot, m):
        rows = pl.ds(pl.multiple_of(m * TM, TM), TM)
        acc[rows, :] += lax.dot_general(rows_v[slot, :, rows], dgu_v[slot], (((0,), (0,)), ((), ())), preferred_element_type=F32)

    def gu_tiles(g, slot, half):
        @pl.loop(half * (NM // 2), (half + 1) * (NM // 2), unroll=UG)
        def _(m):
            gu_tile(slot, m)

        @pl.when(g == last - 1)
        def _():
            put_gu(half).start()

    def compute_first(g):
        slot = g % 2

        @pl.when(g < S)
        def _():
            rest, mine = loads(g, slot)
            rest.wait()
            mine[0].wait()
            act_wait(slot)

            @pl.when(g >= 2)
            def _():
                dgu_store(g - 2, slot).wait()

            for t in range(CHUNK // TA // 2 + CHUNK // TA % 2):
                act_tile(slot, t)

        @pl.when(g >= S)
        def _():
            rest, mine = loads(g, slot)
            rest.wait()
            mine[1].wait()

            @pl.when(g < S + 2)
            def _():
                dgu_store(g - 2, slot).wait()
                dgu_load(g - S, slot).start()

            dgu_load(g - S, slot).wait()

            gu_tiles(g, slot, 0)

    def compute_second(g):
        slot = g % 2

        @pl.when(g < S)
        def _():
            for t in range(CHUNK // TA // 2 + CHUNK // TA % 2, CHUNK // TA):
                act_tile(slot, t)
            dgu_store(g, slot).start()

            @pl.loop(0, 4)
            def _(n):
                down_tile(slot, n)

            @pl.when(g == S - 1)
            def _():
                put_down()

        @pl.when(g >= S)
        def _():
            gu_tiles(g, slot, 1)

    weights = pltpu.make_async_copy(w_down, wd_v, w_sem)
    weights.start()
    greet(peers)
    stage0(jnp.int32(0))
    stage0(jnp.int32(1))
    acc[...] = jnp.zeros_like(acc)
    weights.wait()

    @pl.loop(0, last + 4)
    def _(i):
        @pl.when(i < last)
        def _():
            stage1(i)

        @pl.when(i + 2 < last)
        def _():
            @pl.when(i + 2 >= RING)
            def _():
                drain(i + 2 - RING)

            stage0(i + 2)

        @pl.when(jnp.logical_and(i >= 3, i < last + 3))
        def _():
            stage3(i - 3)

        @pl.when(i >= 4)
        def _():
            compute_first(i - 4)

        @pl.when(jnp.logical_and(i >= 1, i < last + 1))
        def _():
            stage2(i - 1)

        @pl.when(i >= 4)
        def _():
            compute_second(i - 4)

    @pl.loop(last - RING, last)
    def _(g):
        drain(g)

    for half in range(2):
        put_gu(half).wait()


def scatter_kernel(dgu, w_gate, w_up, x, buf, dw_part_in, dx, dw_part, buf_x,
                   acc, x_v, dgu_x, w_v, dgu_v, part_v, sum2, sum1, sum0, core_s, core_r, s3, r3, s2, r2, s1, r1, out_v,
                   ss, rs, xss, xrs, load_sem, x_sem, w_sem, out_sem, put_sem, own_sem):
    me = lax.axis_index("tp")
    peers = peers_of(me)
    ring = 4
    start_x, stage1_x, stage2_x, arrive_x, drain_x = gather_ops(buf_x, xss, xrs, XD, peers)
    x_cols = pl.ds(NM * TM, NB * TM)

    def copy(src, dst, g, k, peer):
        return send(src, dst, ss.at[g % ring, k], rs.at[g % ring, k], peer)

    def to_core(g):
        return copy(core_s.at[g % 2], core_r.at[g % 2], g, 0, peers[3])

    def third(g, d):
        cols = pl.ds(*THIRDS[d])
        return copy(s3.at[g % 2, :, cols], r3.at[g % ring, :, cols], g, 1 + d, peers[d])

    def second(g, q, h):
        cols = pl.ds(*HALVES[h])
        return copy(s2.at[g % 2, q, :, cols], r2.at[g % ring, q, :, cols], g, 4 + 2 * q + h, peers[PAIRS[q][h]])

    def first(g, d):
        return copy(s1.at[g % 2, d], r1.at[g % ring, d], g, 10 + d, peers[d])

    def rows(v):
        return pl.ds(v * R, R)

    def load(g):
        return pltpu.make_async_copy(dgu.at[g], dgu_v.at[g % 2], load_sem.at[g % 2])

    def rest_of_x(src):
        return pltpu.make_async_copy(src.at[pl.ds(R, CHUNK - R), x_cols], x_v.at[pl.ds(R, CHUNK - R)], x_sem.at[2])

    def load_gu(g):
        return (
            pltpu.make_async_copy(dgu.at[g], dgu_x, x_sem.at[0]),
            pltpu.make_async_copy(x.at[pl.ds(pl.multiple_of(g * R, R), R), x_cols], x_v.at[pl.ds(0, R)], x_sem.at[1]),
        )

    def start_gu(g):
        for c in load_gu(g):
            c.start()

        @pl.when(g < S - XD)
        def _():
            rest_of_x(buf.at[S + g]).start()

        @pl.when(g >= S - XD)
        def _():
            rest_of_x(buf_x.at[g - (S - XD)]).start()

    def add_gu(g):
        for c in load_gu(g):
            c.wait()
        rest_of_x(buf_x.at[0]).wait()
        for m in range(NB):
            rows = pl.ds(m * TM, TM)
            acc[rows, :] += lax.dot_general(x_v[:, rows], dgu_x[...], (((0,), (0,)), ((), ())), preferred_element_type=F32)

    def put_gu():
        return pltpu.make_async_copy(acc, dw_part.at[pl.ds(NM * TM, NB * TM)], put_sem)

    def x_own(h):
        return x.at[pl.ds((S - XD + h) * R, R)]

    def keep_own(h):
        return pltpu.make_async_copy(x_own(h), buf_x.at[h, pl.ds(0, R)], own_sem.at[h])

    def put(g):
        return pltpu.make_async_copy(out_v.at[g % 2], dx.at[pl.ds(pl.multiple_of(g * R, R), R)], out_sem.at[g % 2])

    def before(g, waits):
        @pl.when(g >= 2)
        def _():
            for c in waits(g - 2):
                c.wait_send()

    def thirds(g):
        return [third(g, d) for d in range(3)]

    def seconds(g):
        return [second(g, q, h) for q in range(3) for h in range(2)]

    def firsts(g):
        return [first(g, d) for d in range(3)]

    def multiply(g):
        slot = g % 2
        load(g).wait()

        @pl.when(g + 1 < S)
        def _():
            load(g + 1).start()

        before(g, lambda h: [to_core(h)])

        @pl.loop(0, 7, unroll=7)
        def _(n):
            cols = pl.ds(pl.multiple_of(n * 512, 512), 512)
            product = lax.dot_general(dgu_v[slot], w_v[cols, :], (((1,), (1,)), ((), ())), preferred_element_type=F32)
            part_v[:, cols] = product[:HALF]
            core_s[slot, :, cols] = product[HALF:].astype(BF)

        to_core(g).start()

    def add_core(g):
        to_core(g).wait_recv()
        before(g, thirds)

        def both(v):
            return part_v[rows(v), :] + core_r[g % 2, rows(v), :].astype(F32)

        s3[g % 2] = both(XYZ).astype(BF)
        for q, (a, b) in enumerate(PAIRS):
            sum2[g % 2, q] = both(BIT[a] + BIT[b])
        for d in range(3):
            sum1[g % 3, d] = both(BIT[d])
        sum0[g % 4] = both(0)
        for c in thirds(g):
            c.start()

    def add_thirds(g):
        for c in thirds(g):
            c.wait_recv()
        before(g, seconds)
        for q, (a, b) in enumerate(PAIRS):
            d = 3 - a - b
            for e in range(3):
                cols = pl.ds(*THIRDS[e])
                value = sum2[g % 2, q, :, cols]
                if e == d:
                    value = value + r3[g % ring, :, cols].astype(F32)
                s2[g % 2, q, :, cols] = value.astype(BF)
        for c in seconds(g):
            c.start()

    def add_seconds(g):
        for c in seconds(g):
            c.wait_recv()
        before(g, firsts)
        for q, (a, b) in enumerate(PAIRS):
            for h, d in ((0, b), (1, a)):
                cols = pl.ds(*HALVES[h])
                s1[g % 2, d, :, cols] = (sum1[g % 3, d, :, cols] + r2[g % ring, q, :, cols].astype(F32)).astype(BF)
        for c in firsts(g):
            c.start()

    def add_firsts(g):
        for c in firsts(g):
            c.wait_recv()

        @pl.when(g >= 2)
        def _():
            put(g - 2).wait()

        total = sum0[g % 4]
        for d in range(3):
            total = total + r1[g % ring, d].astype(F32)
        out_v[g % 2] = total.astype(BF)
        put(g).start()

    w_copies = [
        pltpu.make_async_copy(w_gate, w_v.at[:, pl.ds(0, FL)], w_sem.at[0]),
        pltpu.make_async_copy(w_up, w_v.at[:, pl.ds(FL, FL)], w_sem.at[1]),
    ]
    for c in w_copies:
        c.start()
    load(jnp.int32(0)).start()
    greet(peers)
    for h in range(XD):
        start_x(h, x_own(h))
        keep_own(h).start()
    acc[...] = jnp.zeros_like(acc)
    for c in w_copies:
        c.wait()

    @pl.loop(0, S + 4)
    def _(i):
        gu_round = jnp.logical_and(i >= LAG, i < S + LAG)

        @pl.when(gu_round)
        def _():
            start_gu(i - LAG)

        for lag, step in ((1, add_core), (2, add_thirds), (3, add_seconds), (4, add_firsts)):
            @pl.when(jnp.logical_and(i >= lag, i < S + lag))
            def _(lag=lag, step=step):
                step(i - lag)

        @pl.when(i < S)
        def _():
            multiply(i)

        @pl.when(gu_round)
        def _():
            add_gu(i - LAG)

        @pl.when(i == S + LAG - 1)
        def _():
            put_gu().start()

        for at, steps in enumerate(X_STEPS):
            @pl.when(i == at)
            def _(steps=steps):
                for step, h in steps:
                    (stage1_x, stage2_x, arrive_x)[step](h)

    for g in (S - 2, S - 1):
        g = jnp.int32(g)
        for c in [to_core(g), *thirds(g), *seconds(g), *firsts(g)]:
            c.wait_send()
        put(g).wait()
    put_gu().wait()
    for h in range(XD):
        drain_x(h)
        keep_own(h).wait()


def finish_kernel(part, dx_in, dw_down_in, *refs):
    xs, dgus, (dx, dw_gate, dw_up, dw_down) = refs[:XD], refs[XD : 2 * XD], refs[2 * XD :]
    dx[...] = dx_in[...]
    dw_down[...] = dw_down_in[...]

    def put(total):
        dw_gate[...] = total[:, :FL].astype(BF)
        dw_up[...] = total[:, FL:].astype(BF)

    @pl.when(pl.program_id(0) * FT < NM * TM)
    def _():
        total = part[...]
        for a, b in zip(xs, dgus):
            total = total + lax.dot_general(a[...], b[...], (((0,), (0,)), ((), ())), preferred_element_type=F32)
        put(total)

    @pl.when(pl.program_id(0) * FT >= NM * TM)
    def _():
        put(part[...])


def solution(mesh):
    any_space = pl.BlockSpec(memory_space=pl.ANY)
    dma = pltpu.SemaphoreType.DMA

    def body(x, dy, gate, up, w_gate, w_up, w_down):
        dgu, dw_part, dw_down, buf = pl.pallas_call(
            gather_kernel,
            out_shape=[
                jax.ShapeDtypeStruct((S, CHUNK, 2 * FL), BF),
                jax.ShapeDtypeStruct((D, 2 * FL), F32),
                jax.ShapeDtypeStruct((FL, D), BF),
                jax.ShapeDtypeStruct((2 * S - XD, CHUNK, D), BF),
            ],
            in_specs=[any_space] * 5,
            out_specs=[any_space] * 4,
            scratch_shapes=[
                pltpu.VMEM((FL, D), BF),
                pltpu.VMEM((NM * TM, 2 * FL), F32),
                pltpu.VMEM((2, CHUNK, D), BF),
                pltpu.VMEM((2, CHUNK, FL), BF),
                pltpu.VMEM((2, CHUNK, FL), BF),
                pltpu.VMEM((2, CHUNK, 2 * FL), BF),
                pltpu.VMEM((FL, CHUNK), BF),
                pltpu.VMEM((2, TM, 2 * FL), BF),
                dma((RING, 20)),
                dma((RING, 20)),
                dma((2, 2)),
                dma((2, 2)),
                dma,
                dma((2,)),
                dma((2, 2)),
            ],
            compiler_params=pltpu.CompilerParams(collective_id=0, has_side_effects=True, vmem_limit_bytes=VMEM_LIMIT),
            name="gather_dy_x",
        )(dy, x, gate, up, w_down)
        dx, dw_part, buf_x = pl.pallas_call(
            scatter_kernel,
            out_shape=[
                jax.ShapeDtypeStruct((S * R, D), BF),
                jax.ShapeDtypeStruct((D, 2 * FL), F32),
                jax.ShapeDtypeStruct((XD, CHUNK, D), BF),
            ],
            in_specs=[any_space] * 6,
            input_output_aliases={5: 1},
            out_specs=[any_space] * 3,
            scratch_shapes=[
                pltpu.VMEM((NB * TM, 2 * FL), F32),
                pltpu.VMEM((CHUNK, NB * TM), BF),
                pltpu.VMEM((CHUNK, 2 * FL), BF),
                pltpu.VMEM((D, 2 * FL), BF),
                pltpu.VMEM((2, CHUNK, 2 * FL), BF),
                pltpu.VMEM((HALF, D), F32),
                pltpu.VMEM((2, 3, R, D), F32),
                pltpu.VMEM((3, 3, R, D), F32),
                pltpu.VMEM((4, R, D), F32),
                pltpu.VMEM((2, HALF, D), BF),
                pltpu.VMEM((2, HALF, D), BF),
                pltpu.VMEM((2, R, D), BF),
                pltpu.VMEM((4, R, D), BF),
                pltpu.VMEM((2, 3, R, D), BF),
                pltpu.VMEM((4, 3, R, D), BF),
                pltpu.VMEM((2, 3, R, D), BF),
                pltpu.VMEM((4, 3, R, D), BF),
                pltpu.VMEM((2, R, D), BF),
                dma((4, 13)),
                dma((4, 13)),
                dma((XD, 20)),
                dma((XD, 20)),
                dma((2,)),
                dma((3,)),
                dma((2,)),
                dma((2,)),
                dma,
                dma((XD,)),
            ],
            compiler_params=pltpu.CompilerParams(collective_id=1, has_side_effects=True, vmem_limit_bytes=VMEM_LIMIT),
            name="scatter_dx",
        )(dgu, w_gate, w_up, x, buf, dw_part)
        by_rows, x_cols = pl.BlockSpec((FT, FL), lambda m: (m, 0)), FT
        dx_spec = pl.BlockSpec((S * R, x_cols), lambda m: (0, m))
        down_spec = pl.BlockSpec((FL, x_cols), lambda m: (0, m))
        dx, dw_gate, dw_up, dw_down = pl.pallas_call(
            finish_kernel,
            grid=(D // FT,),
            out_shape=[
                jax.ShapeDtypeStruct((S * R, D), BF),
                jax.ShapeDtypeStruct((D, FL), BF),
                jax.ShapeDtypeStruct((D, FL), BF),
                jax.ShapeDtypeStruct((FL, D), BF),
            ],
            in_specs=[pl.BlockSpec((FT, 2 * FL), lambda m: (m, 0)), dx_spec, down_spec]
            + [pl.BlockSpec((None, CHUNK, FT), lambda m, h=h: (h, 0, jnp.minimum(m, NM * TM // FT - 1))) for h in range(XD)]
            + [pl.BlockSpec((None, CHUNK, 2 * FL), lambda m, h=h: (S - XD + h, 0, 0)) for h in range(XD)],
            out_specs=[dx_spec, by_rows, by_rows, down_spec],
            compiler_params=pltpu.CompilerParams(vmem_limit_bytes=VMEM_LIMIT),
            name="finish_dw",
        )(dw_part, dx, dw_down, *[buf_x] * XD, *[dgu] * XD)
        return dx, dw_gate, dw_up, dw_down

    rows, cols = P(("dp", "tp"), None), P("dp", "tp")
    return jax.shard_map(
        body,
        mesh=mesh,
        in_specs=(rows, rows, cols, cols, P(None, "tp"), P(None, "tp"), P("tp", None)),
        out_specs=(rows, cols, cols, rows),
        check_vma=False,
    )
```
